32 devices in a mesh: row: 4 (over x, core), col: 4 (over z), depth: 2 (over y).
Axes of the slice: x: 2, y: 2, z: 4, core: 2. Of those that a mesh axis runs over, the one named last changes fastest.
Arguments:
- tokens: bfloat16 [512, 4096], P(('col', 'depth'), 'row'), may hold values from -6 to 6
- w_gate: bfloat16 [4096, 14336], P('row', 'col'), may hold values from -0.09375 to 0.09375
- w_up: bfloat16 [4096, 14336], P('row', 'col'), may hold values from -0.09375 to 0.09375
- w_down: bfloat16 [14336, 4096], P('col', 'row'), may hold values from -0.046875 to 0.046875
- cotangent: bfloat16 [512, 4096], P(('col', 'depth'), 'row'), may hold values from -0.25 to 0.25
Outputs:
- mixed: bfloat16 [512, 4096], P(('col', 'depth'), 'row')
- grad_gate: bfloat16 [4096, 14336], P(('row', 'depth'), 'col')
- grad_up: bfloat16 [4096, 14336], P(('row', 'depth'), 'col')
- grad_down: bfloat16 [14336, 4096], P(('col', 'depth'), 'row')
The draws below stay inside these ranges and needn't reach their ends.
All inputs are finite; a program needn't handle non-finite values.
Results may differ from the reference program's by a relative error of at most 0.025.
Values may be sent and summed in bfloat16 or wider, within the bound.
No kernel may reach another device: no remote copies, remote signals or barrier semaphores. Data moves between devices by JAX's collectives and lax.ppermute only.
A program may use at most 128 MiB of HBM per device.

```python
import jax
import jax.numpy as jnp
from jax import lax

D = 4096
FF = 14336
TOK_DEV = 64
TOKENS = 512
N_ROW = 4
N_COL = 4
N_DEPTH = 2


def steps_of(own_key, shape, pieces, low, top_value):
    level, own = 1.0, jax.random.fold_in(own_key, 6)
    for axis_at, parts in pieces:
        draws = jnp.exp(jax.random.uniform(jax.random.fold_in(own, axis_at), (parts,), jnp.float32, low / len(pieces), top_value / len(pieces)))
        level = level * jnp.repeat(draws, shape[axis_at] // parts).reshape([-1 if axis == axis_at else 1 for axis in range(len(shape))])
    return level


def noise(stream_key, shape, width, reach, split=(), kind=jnp.bfloat16):
    gain = steps_of(stream_key, shape, split, -0.22, 0.18) if split else 1.0
    values = jax.random.normal(stream_key, shape, jnp.float32) * width * gain
    return jnp.minimum(jnp.maximum(values, -reach), reach).astype(kind)


def setup_inputs(seed: int = 0) -> dict:
    splits = jax.random.split(jax.random.key(seed), 6)
    tokens = noise(splits[0], (TOKENS, D), 1.0, 6.0, ((0, 8), (1, 4)))
    w_gate = noise(splits[1], (D, FF), D ** -0.5, 0.09375, ((0, 4), (1, 4)))
    w_up = noise(splits[2], (D, FF), D ** -0.5, 0.09375, ((0, 4), (1, 4)))
    w_down = noise(splits[3], (FF, D), FF ** -0.5, 0.046875, ((0, 4), (1, 4)))
    cotangent = noise(splits[4], (TOKENS, D), (TOKENS ** -0.5), 0.25, ((0, 8), (1, 4)))
    return dict(tokens=tokens, w_gate=w_gate, w_up=w_up, w_down=w_down, cotangent=cotangent)


COLS_CONTRACT = (((1,), (1,)), ((), ()))
ROWS_CONTRACT = (((0,), (0,)), ((), ()))


def rounded_add(running, addend):
    rounded = lax.optimization_barrier(addend.astype(jnp.bfloat16))
    return running + rounded.astype(jnp.float32)


def layer_rows(array, layer_index):
    shaped = array.reshape(N_COL, N_DEPTH, TOK_DEV, array.shape[1])
    return shaped[:, layer_index].reshape(N_COL * TOK_DEV, array.shape[1])


def reference(tokens, w_gate, w_up, w_down, cotangent):
    feat_width = D // N_ROW
    token_count = tokens.shape[0]
    gate_sum = jnp.zeros((token_count, FF), jnp.float32)
    up_sum = jnp.zeros((token_count, FF), jnp.float32)
    hidden_grad = jnp.zeros((token_count, FF), jnp.float32)
    for block_index in range(N_ROW):
        lower_edge = block_index * feat_width
        upper_edge = lower_edge + feat_width
        tok_block = tokens[:, lower_edge:upper_edge]
        gate_sum = rounded_add(gate_sum, jnp.dot(tok_block, w_gate[lower_edge:upper_edge], preferred_element_type=jnp.float32))
        up_sum = rounded_add(up_sum, jnp.dot(tok_block, w_up[lower_edge:upper_edge], preferred_element_type=jnp.float32))
        hidden_grad = rounded_add(hidden_grad, lax.dot_general(cotangent[:, lower_edge:upper_edge], w_down[:, lower_edge:upper_edge], COLS_CONTRACT, preferred_element_type=jnp.float32))
    hidden = (jax.nn.silu(gate_sum) * up_sum).astype(jnp.bfloat16)
    mixed = jnp.dot(hidden, w_down, preferred_element_type=jnp.float32).astype(jnp.bfloat16)
    sigmoid_gate = jax.nn.sigmoid(gate_sum)
    d_gate = (hidden_grad * up_sum * sigmoid_gate * (1.0 + gate_sum * (1.0 - sigmoid_gate))).astype(jnp.bfloat16)
    d_up = (hidden_grad * gate_sum * sigmoid_gate).astype(jnp.bfloat16)
    grad_gate = jnp.zeros((D, FF), jnp.float32)
    grad_up = jnp.zeros((D, FF), jnp.float32)
    grad_down = jnp.zeros((FF, D), jnp.float32)
    for layer_index in range(N_DEPTH):
        tok_layer = layer_rows(tokens, layer_index)
        grad_gate = rounded_add(grad_gate, lax.dot_general(tok_layer, layer_rows(d_gate, layer_index), ROWS_CONTRACT, preferred_element_type=jnp.float32))
        grad_up = rounded_add(grad_up, lax.dot_general(tok_layer, layer_rows(d_up, layer_index), ROWS_CONTRACT, preferred_element_type=jnp.float32))
        grad_down = rounded_add(grad_down, lax.dot_general(layer_rows(hidden, layer_index), layer_rows(cotangent, layer_index), ROWS_CONTRACT, preferred_element_type=jnp.float32))
    return (mixed, grad_gate.astype(jnp.bfloat16), grad_up.astype(jnp.bfloat16), grad_down.astype(jnp.bfloat16))
```

```python
import jax
import jax.numpy as jnp
from jax import lax
from jax.sharding import PartitionSpec as P

COLS_CONTRACT = (((1,), (1,)), ((), ()))
ROWS_CONTRACT = (((0,), (0,)), ((), ()))


def gate_grads(hidden_grad, gate_sum, up_sum):
    sigmoid_gate = jax.nn.sigmoid(gate_sum)
    d_gate = (hidden_grad * up_sum * sigmoid_gate * (1.0 + gate_sum * (1.0 - sigmoid_gate))).astype(
        jnp.bfloat16
    )
    d_up = (hidden_grad * gate_sum * sigmoid_gate).astype(jnp.bfloat16)
    return (d_gate, d_up)


def gathered(tokens, w_gate, w_up, w_down, cotangent):
    hid_width = w_gate.shape[1]
    token_rows = lax.all_gather(tokens, "col", axis=0, tiled=True)
    row_piece = token_rows
    joined = lax.psum_scatter(
        jnp.concatenate(
            [
                jnp.dot(row_piece, w_gate, preferred_element_type=jnp.float32),
                jnp.dot(row_piece, w_up, preferred_element_type=jnp.float32),
            ],
            axis=1,
        ).astype(jnp.bfloat16),
        "row",
        scatter_dimension=0,
        tiled=True,
    ).astype(jnp.float32)
    gate_sum = joined[:, :hid_width]
    up_sum = joined[:, hid_width:]
    hidden = (jax.nn.silu(gate_sum) * up_sum).astype(jnp.bfloat16)
    hidden_rows = lax.all_gather(hidden, "row", axis=0, tiled=True)
    row_piece = hidden_rows
    mixed = lax.psum_scatter(
        jnp.dot(row_piece, w_down, preferred_element_type=jnp.float32).astype(jnp.bfloat16),
        "col",
        scatter_dimension=0,
        tiled=True,
    )
    cot_rows = lax.all_gather(cotangent, "col", axis=0, tiled=True)
    row_piece = cot_rows
    hidden_grad = lax.psum_scatter(
        lax.dot_general(
            row_piece, w_down, COLS_CONTRACT, preferred_element_type=jnp.float32
        ).astype(jnp.bfloat16),
        "row",
        scatter_dimension=0,
        tiled=True,
    ).astype(jnp.float32)
    d_gate, d_up = gate_grads(hidden_grad, gate_sum, up_sum)
    d_gate_rows, d_up_rows = (
        lax.all_gather(d_gate, "row", axis=0, tiled=True),
        lax.all_gather(d_up, "row", axis=0, tiled=True),
    )
    down_term = lax.dot_general(
        hidden_rows, cot_rows, ROWS_CONTRACT, preferred_element_type=jnp.float32
    )
    grad_down = lax.psum_scatter(
        down_term.astype(jnp.bfloat16), "depth", scatter_dimension=0, tiled=True
    )
    layer_tokens = lax.all_to_all(token_rows, "depth", split_axis=1, concat_axis=0, tiled=True)
    block_rows = token_rows.shape[0]
    empty_grad = jnp.zeros((layer_tokens.shape[1], d_gate_rows.shape[1]), jnp.float32)
    first_row = jnp.int32(0)
    gate_total = empty_grad
    up_total = empty_grad
    gate_piece = lax.all_gather(d_gate_rows, "depth", axis=0, tiled=True)
    up_piece = lax.all_gather(d_up_rows, "depth", axis=0, tiled=True)
    for sub_index in range(gate_piece.shape[0] // block_rows):
        gate_block = gate_piece[sub_index * block_rows : (sub_index + 1) * block_rows]
        up_block = up_piece[sub_index * block_rows : (sub_index + 1) * block_rows]
        offset = first_row + sub_index * block_rows
        tok_block = lax.dynamic_slice_in_dim(layer_tokens, offset, block_rows, 0)
        gate_part = lax.optimization_barrier(
            lax.dot_general(
                tok_block, gate_block, ROWS_CONTRACT, preferred_element_type=jnp.float32
            ).astype(jnp.bfloat16)
        )
        up_part = lax.optimization_barrier(
            lax.dot_general(
                tok_block, up_block, ROWS_CONTRACT, preferred_element_type=jnp.float32
            ).astype(jnp.bfloat16)
        )
        gate_total = gate_total + gate_part.astype(jnp.float32)
        up_total = up_total + up_part.astype(jnp.float32)
    return (mixed, gate_total.astype(jnp.bfloat16), up_total.astype(jnp.bfloat16), grad_down)


def swap(value, axis, size, step):
    return lax.ppermute(value, axis, [(at, (at + step) % size) for at in range(size)])


def partner(value, size, bit):
    return lax.ppermute(value, "row", [(at, at ^ bit) for at in range(size)])


def paired(tokens, w_gate, w_up, w_down, cotangent):
    n_row, n_col, n_depth = (lax.axis_size(name) for name in ("row", "col", "depth"))
    depth = lax.axis_index("depth")
    even = lax.axis_index("row") % 2 == 0
    first = depth == 0
    rows, feats = tokens.shape
    half = w_gate.shape[1] // n_depth

    def order(own, other):
        return jnp.concatenate([jnp.where(even, own, other), jnp.where(even, other, own)], axis=0)

    def halves(value):
        return value[:rows], value[rows:]

    w_in = jnp.concatenate(
        [
            lax.dynamic_slice_in_dim(w_gate, depth * half, half, 1),
            lax.dynamic_slice_in_dim(w_up, depth * half, half, 1),
        ],
        axis=1,
    )
    w_out = lax.dynamic_slice_in_dim(w_down, depth * half, half, 0)

    tok = {0: order(tokens, swap(tokens, "depth", n_depth, 1))}
    cot = {0: order(cotangent, swap(cotangent, "depth", n_depth, 1))}
    steps = [0]
    for step in range(1, n_col):
        near, back = (step + 1) // 2, step % 2 == 0
        at = n_col - near if back else near
        source = (at + 1) % n_col if back else at - 1
        tok[at] = swap(tok[source], "col", n_col, -1 if back else 1)
        cot[at] = swap(cot[source], "col", n_col, -1 if back else 1)
        steps.append(at)

    mixed = None
    hidden_all, gate_all, up_all = [], [], []
    for at in steps:
        joined = jnp.dot(tok[at], w_in, preferred_element_type=jnp.float32).astype(jnp.bfloat16)
        back = lax.dot_general(
            cot[at], w_out, COLS_CONTRACT, preferred_element_type=jnp.float32
        ).astype(jnp.bfloat16)
        joined_keep, joined_send = halves(joined)
        back_keep, back_send = halves(back)
        joined_mine = joined_keep + partner(joined_send, n_row, 1)
        back_mine = back_keep + partner(back_send, n_row, 1)
        joined_sum = joined_mine.astype(jnp.float32) + partner(joined_mine, n_row, 2).astype(jnp.float32)
        hidden_grad = back_mine.astype(jnp.float32) + partner(back_mine, n_row, 2).astype(jnp.float32)
        gate_sum, up_sum = joined_sum[:, :half], joined_sum[:, half:]
        hidden = (jax.nn.silu(gate_sum) * up_sum).astype(jnp.bfloat16)
        d_gate, d_up = gate_grads(hidden_grad, gate_sum, up_sum)

        hidden_rows = jnp.concatenate([hidden, partner(hidden, n_row, 1)], axis=0)
        hidden_all.append(hidden_rows)
        part = jnp.dot(hidden_rows, w_out, preferred_element_type=jnp.float32).astype(jnp.bfloat16)
        low, high = halves(part)
        own, other = jnp.where(even, low, high), jnp.where(even, high, low)
        term = own.astype(jnp.float32) + swap(other, "depth", n_depth, 1).astype(jnp.float32)
        if at:
            term = swap(term.astype(jnp.bfloat16), "col", n_col, -at).astype(jnp.float32)
        mixed = term if mixed is None else mixed + term

        for grad, rows_all in ((d_gate, gate_all), (d_up, up_all)):
            across = swap(grad, "depth", n_depth, 1)
            mine = jnp.concatenate([grad, partner(grad, n_row, 1)], axis=0)
            theirs = jnp.concatenate([partner(across, n_row, 1), across], axis=0)
            rows_all.append(
                jnp.concatenate(
                    [jnp.where(first, mine, theirs), jnp.where(first, theirs, mine)], axis=1
                )
            )

    def total(left, right):
        return lax.dot_general(
            left, right, ROWS_CONTRACT, preferred_element_type=jnp.float32
        ).astype(jnp.bfloat16)

    tok_all = jnp.concatenate([tok[at] for at in steps], axis=0)
    cot_all = jnp.concatenate([cot[at] for at in steps], axis=0)
    width = feats // n_depth
    tok_part = lax.dynamic_slice_in_dim(tok_all, depth * width, width, 1)
    grad_down = total(jnp.concatenate(hidden_all, axis=0), cot_all)
    grad_gate = total(tok_part, jnp.concatenate(gate_all, axis=0))
    grad_up = total(tok_part, jnp.concatenate(up_all, axis=0))
    return (mixed.astype(jnp.bfloat16), grad_gate, grad_up, grad_down)


def solution(mesh):
    fits = mesh.shape["row"] == 4 and mesh.shape["depth"] == 2
    per_device = paired if fits else gathered
    placed = (
        P(("col", "depth"), "row"),
        P("row", "col"),
        P("row", "col"),
        P("col", "row"),
        P(("col", "depth"), "row"),
    )
    return jax.shard_map(
        per_device,
        mesh=mesh,
        in_specs=placed,
        out_specs=(
            P(("col", "depth"), "row"),
            P(("row", "depth"), "col"),
            P(("row", "depth"), "col"),
            P(("col", "depth"), "row"),
        ),
        check_vma=False,
    )
```

```python
import jax
import jax.numpy as jnp
from jax import lax
from jax.sharding import PartitionSpec as P


COLS_CONTRACT = (((1,), (1,)), ((), ()))
ROWS_CONTRACT = (((0,), (0,)), ((), ()))


def gate_grads(hidden_grad, gate_sum, up_sum):
    sigmoid_gate = jax.nn.sigmoid(gate_sum)
    d_gate = (hidden_grad * up_sum * sigmoid_gate * (1.0 + gate_sum * (1.0 - sigmoid_gate))).astype(
        jnp.bfloat16
    )
    d_up = (hidden_grad * gate_sum * sigmoid_gate).astype(jnp.bfloat16)
    return (d_gate, d_up)


def gathered(tokens, w_gate, w_up, w_down, cotangent):
    hid_width = w_gate.shape[1]
    token_rows = lax.all_gather(tokens, "col", axis=0, tiled=True)
    row_piece = token_rows
    joined = lax.psum_scatter(
        jnp.concatenate(
            [
                jnp.dot(row_piece, w_gate, preferred_element_type=jnp.float32),
                jnp.dot(row_piece, w_up, preferred_element_type=jnp.float32),
            ],
            axis=1,
        ).astype(jnp.bfloat16),
        "row",
        scatter_dimension=0,
        tiled=True,
    ).astype(jnp.float32)
    gate_sum = joined[:, :hid_width]
    up_sum = joined[:, hid_width:]
    hidden = (jax.nn.silu(gate_sum) * up_sum).astype(jnp.bfloat16)
    hidden_rows = lax.all_gather(hidden, "row", axis=0, tiled=True)
    row_piece = hidden_rows
    mixed = lax.psum_scatter(
        jnp.dot(row_piece, w_down, preferred_element_type=jnp.float32).astype(jnp.bfloat16),
        "col",
        scatter_dimension=0,
        tiled=True,
    )
    cot_rows = lax.all_gather(cotangent, "col", axis=0, tiled=True)
    row_piece = cot_rows
    hidden_grad = lax.psum_scatter(
        lax.dot_general(
            row_piece, w_down, COLS_CONTRACT, preferred_element_type=jnp.float32
        ).astype(jnp.bfloat16),
        "row",
        scatter_dimension=0,
        tiled=True,
    ).astype(jnp.float32)
    d_gate, d_up = gate_grads(hidden_grad, gate_sum, up_sum)
    d_gate_rows, d_up_rows = (
        lax.all_gather(d_gate, "row", axis=0, tiled=True),
        lax.all_gather(d_up, "row", axis=0, tiled=True),
    )
    down_term = lax.dot_general(
        hidden_rows, cot_rows, ROWS_CONTRACT, preferred_element_type=jnp.float32
    )
    grad_down = lax.psum_scatter(
        down_term.astype(jnp.bfloat16), "depth", scatter_dimension=0, tiled=True
    )
    layer_tokens = lax.all_to_all(token_rows, "depth", split_axis=1, concat_axis=0, tiled=True)
    block_rows = token_rows.shape[0]
    empty_grad = jnp.zeros((layer_tokens.shape[1], d_gate_rows.shape[1]), jnp.float32)
    first_row = jnp.int32(0)
    gate_total = empty_grad
    up_total = empty_grad
    gate_piece = lax.all_gather(d_gate_rows, "depth", axis=0, tiled=True)
    up_piece = lax.all_gather(d_up_rows, "depth", axis=0, tiled=True)
    for sub_index in range(gate_piece.shape[0] // block_rows):
        gate_block = gate_piece[sub_index * block_rows : (sub_index + 1) * block_rows]
        up_block = up_piece[sub_index * block_rows : (sub_index + 1) * block_rows]
        offset = first_row + sub_index * block_rows
        tok_block = lax.dynamic_slice_in_dim(layer_tokens, offset, block_rows, 0)
        gate_part = lax.optimization_barrier(
            lax.dot_general(
                tok_block, gate_block, ROWS_CONTRACT, preferred_element_type=jnp.float32
            ).astype(jnp.bfloat16)
        )
        up_part = lax.optimization_barrier(
            lax.dot_general(
                tok_block, up_block, ROWS_CONTRACT, preferred_element_type=jnp.float32
            ).astype(jnp.bfloat16)
        )
        gate_total = gate_total + gate_part.astype(jnp.float32)
        up_total = up_total + up_part.astype(jnp.float32)
    return (mixed, gate_total.astype(jnp.bfloat16), up_total.astype(jnp.bfloat16), grad_down)


def swap(value, axis, size, step):
    return lax.ppermute(value, axis, [(at, (at + step) % size) for at in range(size)])


def partner(value, size, bit):
    return lax.ppermute(value, "row", [(at, at ^ bit) for at in range(size)])


def bf16_dot(left, right, dims):
    return lax.dot_general(left, right, dims, preferred_element_type=jnp.float32).astype(
        jnp.bfloat16
    )


MATMUL = (((1,), (0,)), ((), ()))


def paired(tokens, w_gate, w_up, w_down, cotangent):
    n_row, n_col, n_depth = (lax.axis_size(name) for name in ("row", "col", "depth"))
    depth = lax.axis_index("depth")
    even = lax.axis_index("row") % 2 == 0
    first = depth == 0
    rows, feats = tokens.shape
    half = w_gate.shape[1] // n_depth

    own = jnp.stack([tokens, cotangent])
    other = swap(own, "depth", n_depth, 1)
    pair = {
        0: jnp.concatenate([jnp.where(even, own, other), jnp.where(even, other, own)], axis=1)
    }
    groups = [0]
    for step in range(1, n_col):
        near, back = (step + 1) // 2, step % 2 == 0
        at = n_col - near if back else near
        source = (at + 1) % n_col if back else at - 1
        pair[at] = [swap(pair[source][part], "col", n_col, -1 if back else 1) for part in range(2)]
        groups.append(at)

    my_gate, my_up = lax.optimization_barrier(
        (
            lax.dynamic_slice_in_dim(w_gate, depth * half, half, 1),
            lax.dynamic_slice_in_dim(w_up, depth * half, half, 1),
        )
    )
    my_down = lax.dynamic_slice_in_dim(w_down, depth * half, half, 0)

    mixed = None
    hidden_all, tok_all, cot_all, grads_all = [], [], [], []
    for at in groups:
        tok, cot = pair[at][0], pair[at][1]
        tok_all.append(tok)
        cot_all.append(cot)
        inner = [bf16_dot(tok, my_gate, MATMUL), bf16_dot(tok, my_up, MATMUL)]
        mine = jnp.stack([term[:rows] for term in inner])
        rest = partner(jnp.stack([term[rows:] for term in inner]), n_row, 1)
        mine = mine + rest
        sums = mine.astype(jnp.float32) + partner(mine, n_row, 2).astype(jnp.float32)
        gate_sum, up_sum = sums[0], sums[1]
        back = bf16_dot(cot, my_down, COLS_CONTRACT)
        rest = partner(back[rows:], n_row, 1)
        mine = back[:rows] + rest
        hidden_grad = mine.astype(jnp.float32) + partner(mine, n_row, 2).astype(jnp.float32)
        hidden = (jax.nn.silu(gate_sum) * up_sum).astype(jnp.bfloat16)
        d_gate, d_up = gate_grads(hidden_grad, gate_sum, up_sum)
        grads = jnp.stack([d_gate, d_up])
        across = swap(grads, "depth", n_depth, 1)
        beside = partner(jnp.stack([d_gate, d_up, hidden]), n_row, 1)

        hidden_rows = jnp.concatenate([hidden, beside[2]], axis=0)
        hidden_all.append(hidden_rows)
        part = bf16_dot(hidden_rows, my_down, MATMUL)
        low, high = part[:rows], part[rows:]
        term = jnp.where(even, low, high).astype(jnp.float32) + swap(
            jnp.where(even, high, low), "depth", n_depth, 1
        ).astype(jnp.float32)
        if at:
            term = swap(term.astype(jnp.bfloat16), "col", n_col, -at).astype(jnp.float32)
        mixed = term if mixed is None else mixed + term

        near_cols = jnp.concatenate([grads, beside[:2]], axis=1)
        far_cols = jnp.concatenate([partner(across, n_row, 1), across], axis=1)
        grads_all.append(
            jnp.concatenate(
                [jnp.where(first, near_cols, far_cols), jnp.where(first, far_cols, near_cols)],
                axis=2,
            )
        )

    tok_all = jnp.concatenate(tok_all, axis=0)
    cot_all = jnp.concatenate(cot_all, axis=0)
    width = feats // n_depth
    tok_part = lax.dynamic_slice_in_dim(tok_all, depth * width, width, 1)
    grad_down = bf16_dot(jnp.concatenate(hidden_all, axis=0), cot_all, ROWS_CONTRACT)
    gate_rows, up_rows, tok_part = lax.optimization_barrier(
        (
            jnp.concatenate([block[0] for block in grads_all], axis=0),
            jnp.concatenate([block[1] for block in grads_all], axis=0),
            tok_part,
        )
    )
    grad_gate = bf16_dot(tok_part, gate_rows, ROWS_CONTRACT)
    grad_up = bf16_dot(tok_part, up_rows, ROWS_CONTRACT)
    return (mixed.astype(jnp.bfloat16), grad_gate, grad_up, grad_down)


def solution(mesh):
    fits = mesh.shape["row"] == 4 and mesh.shape["depth"] == 2

    def per_device(*arrays):
        return paired(*arrays) if fits else gathered(*arrays)

    placed = (
        P(("col", "depth"), "row"),
        P("row", "col"),
        P("row", "col"),
        P("col", "row"),
        P(("col", "depth"), "row"),
    )
    return jax.shard_map(
        per_device,
        mesh=mesh,
        in_specs=placed,
        out_specs=(
            P(("col", "depth"), "row"),
            P(("row", "depth"), "col"),
            P(("row", "depth"), "col"),
            P(("col", "depth"), "row"),
        ),
        check_vma=False,
    )
```
